256 devices in a mesh: seq: 32 (over y, z), ch: 8 (over x, core).
Axes of the slice: x: 4, y: 4, z: 8, core: 2. Of those that a mesh axis runs over, the one named last changes fastest.
Arguments:
- tokens: bfloat16 [4096, 4096], P('seq', 'ch'), may hold values from -6 to 6
- norm_gain: float32 [4096], replicated, may hold values from 0.5 to 1.5
- in_proj: bfloat16 [4096, 2, 8192], P('seq', None, 'ch'), may hold values from -0.09375 to 0.09375
- conv_weight: float32 [4, 8192], P(None, 'ch'), may hold values from -3 to 3
- conv_bias: float32 [8192], P('ch'), may hold values from -2 to 2
- x_proj: bfloat16 [8192, 544], P('ch'), may hold values from -0.0625 to 0.0625
- dt_proj: bfloat16 [512, 8192], P(None, 'ch'), may hold values from -0.25 to 0.25
- dt_bias: float32 [8192], P('ch'), may hold values from -4 to 1
- a_log: float32 [8192, 16], P('ch'), as said below
- d_skip: float32 [8192], P('ch'), may hold values from -32 to 32
- out_proj: bfloat16 [8192, 4096], P('ch', 'seq'), may hold values from -0.0625 to 0.0625
Outputs:
- mixed: bfloat16 [4096, 4096], P('seq', 'ch')
The draws below stay inside these ranges and needn't reach their ends.
Inputs may be any that keep to these rules, and one draw needn't show every extreme that they name: Every entry of a_log lies between ln(0.2 / 4096) and ln(0.2).
All inputs are finite; a program needn't handle non-finite values.
Results may differ from the reference program's by a relative error of at most 0.014.
Values may be sent and summed in bfloat16 or wider, within the bound.
No kernel may reach another device: no remote copies, remote signals or barrier semaphores. Data moves between devices by JAX's collectives and lax.ppermute only.
A program may use at most 64 MiB of HBM per device.

```python
import math
import jax
import jax.numpy as jnp
from jax import lax

D = 4096
E = 8192
R = 512
N = 16
TOKENS = 4096
N_CH = 8


def draw_a_log(key, part):
    key_kind, key_place = jax.random.split(jax.random.fold_in(key, 17))
    share = 0.5
    chosen = jax.random.uniform(key_kind, (E, N), jnp.float32) < share
    where_in = jax.random.uniform(key_place, (E, N), jnp.float32)
    lowest = math.log(0.2 / TOKENS)
    middle = math.log(1.0 / TOKENS)
    highest = math.log(0.2)
    slower = lowest + where_in * (middle - lowest)
    faster = middle + where_in * (highest - middle)
    return jnp.where(chosen, slower, faster).astype(jnp.float32)


def draw_d_skip(key, part):
    key_size = jax.random.fold_in(jax.random.fold_in(key, 29), 0)
    where_in = jax.random.uniform(key_size, (E,), jnp.float32)
    values = 0.5 + where_in
    return values.astype(jnp.float32)


def block_scale(stream_key, shape, cuts, least, largest):
    def one(dim, blocks):
        draws = jax.random.uniform(jax.random.fold_in(jax.random.fold_in(stream_key, 6), dim), (blocks,), jnp.float32, least / len(cuts), largest / len(cuts))
        return jnp.repeat(jnp.exp(draws), shape[dim] // blocks).reshape((-1,) + (1,) * (len(shape) - dim - 1))

    level = one(*cuts[0])
    for cut in cuts[1:]:
        level = level * one(*cut)
    return level


def scatter_about(stream_key, extent, width, reach, cuts=(), held_as=jnp.bfloat16):
    factor_of = block_scale(stream_key, extent, cuts, -0.22, 0.18) if cuts else 1.0
    entries = jax.random.normal(stream_key, extent, jnp.float32) * width * factor_of
    return jnp.minimum(jnp.maximum(entries, -reach), reach).astype(held_as)


def setup_inputs(seed: int = 0) -> dict:
    key_of = jax.random.split(jax.random.key(seed), 12)
    return {
        "tokens": scatter_about(key_of[0], (TOKENS, D), 1.0, 6.0, ((0, 32), (1, 8))),
        "norm_gain": jnp.clip(1.0 + 0.1 * jax.random.normal(key_of[1], (D,), jnp.float32), 0.5, 1.5),
        "in_proj": scatter_about(key_of[2], (D, 2, E), D ** -0.5, 0.09375, ((0, 32), (2, 8))),
        "conv_weight": scatter_about(key_of[3], (4, E), 0.5, 3.0, ((1, 8),), jnp.float32),
        "conv_bias": scatter_about(key_of[4], (E,), 0.3, 2.0, ((0, 8),), jnp.float32),
        "x_proj": scatter_about(key_of[5], (E, R + 2 * N), E ** -0.5, 0.0625, ((0, 8),)),
        "dt_proj": scatter_about(key_of[6], (R, E), R ** -0.5, 0.25, ((1, 8),)),
        "dt_bias": jnp.clip(-4.0 + 5.0 * jax.random.uniform(key_of[7], (E,), jnp.float32) ** block_scale(key_of[7], (E,), ((0, 8),), -0.2, 0.2), -4.0, 1.0),
        "a_log": draw_a_log(jax.random.fold_in(key_of[11], 71), 0),
        "d_skip": draw_d_skip(jax.random.fold_in(key_of[11], 71), 0),
        "out_proj": scatter_about(key_of[10], (E, D), E ** -0.5, 0.0625, ((0, 8), (1, 32))),
    }


def reference(tokens, norm_gain, in_proj, conv_weight, conv_bias, x_proj, dt_proj, dt_bias, a_log, d_skip, out_proj):
    tokens_wide = tokens.astype(jnp.float32)
    scale_rows = lax.rsqrt(lax.optimization_barrier(jnp.mean(tokens_wide * tokens_wide, axis=-1, keepdims=True)) + 1e-06)
    normed = (tokens_wide * scale_rows * norm_gain).astype(jnp.bfloat16)
    both = jnp.dot(normed, in_proj.reshape(D, 2 * E), preferred_element_type=jnp.float32)
    conv_input = both[:, :E].astype(jnp.bfloat16)
    gate = both[:, E:].astype(jnp.bfloat16)
    padded = jnp.concatenate([jnp.zeros((3, E), jnp.bfloat16), conv_input], 0).astype(jnp.float32)
    convolved = conv_bias + conv_weight[0] * padded[0:TOKENS]
    for tap in range(1, 4):
        convolved = convolved + conv_weight[tap] * padded[tap:tap + TOKENS]
    activated = jax.nn.silu(convolved)
    features = jnp.dot(activated.astype(jnp.bfloat16), x_proj, preferred_element_type=jnp.float32)
    step_raw = features[:, :R].astype(jnp.bfloat16)
    b_matrix = features[:, R:R + N]
    c_matrix = features[:, R + N:]
    step_size = jax.nn.softplus(jnp.dot(step_raw, dt_proj, preferred_element_type=jnp.float32) + dt_bias)
    a_matrix = -jnp.exp(a_log)

    def advance(state, inputs):
        step_now, act_now, b_now, c_now = inputs
        state = jnp.exp(step_now[:, None] * a_matrix) * state + (step_now * act_now)[:, None] * b_now[None, :]
        return (state, lax.optimization_barrier(jnp.sum(state * c_now[None, :], axis=1)))
    _, outputs_ssm = lax.scan(advance, jnp.zeros((E, N), jnp.float32), (step_size, activated, b_matrix, c_matrix))
    scanned = outputs_ssm + d_skip * activated
    gated = (scanned * jax.nn.silu(gate.astype(jnp.float32))).astype(jnp.bfloat16)
    group_width = E // N_CH
    running = jnp.zeros((TOKENS, D), jnp.float32)
    for group in range(N_CH):
        partial_value = jnp.dot(gated[:, group * group_width:(group + 1) * group_width], out_proj[group * group_width:(group + 1) * group_width], preferred_element_type=jnp.float32).astype(jnp.bfloat16)
        partial_value = lax.optimization_barrier(partial_value)
        running = running + partial_value.astype(jnp.float32)
    return running.astype(jnp.bfloat16)
```

```python
import functools

import jax
import jax.numpy as jnp
from jax import lax
from jax.experimental import pallas as pl
from jax.experimental.pallas import tpu as pltpu
from jax.sharding import Mesh
from jax.sharding import PartitionSpec as P


SEQ = ("y", "z")
CH = ("x", "c")
HALO = 16
AXES = ("y", "z", "x", "c")
Y, Z, X, C = range(4)
LOG2E = 1.4426950408889634


def shifted(block, axis, distance):
    n = lax.axis_size(axis)
    return lax.ppermute(block, axis, [(i, (i + distance) % n) for i in range(n)])


def from_behind(block, axis):
    return [block] + [shifted(block, axis, k) for k in range(1, lax.axis_size(axis))]


def given_back(pieces, axis):
    return [pieces[0]] + [shifted(pieces[k], axis, -k) for k in range(1, len(pieces))]


def place():
    return jnp.stack([lax.axis_index(axis) for axis in AXES]).astype(jnp.int32)


def call(kernel, out_shape, *operands, scratch=()):
    whole = pl.BlockSpec(memory_space=pltpu.VMEM)
    return pl.pallas_call(
        kernel,
        out_shape=out_shape,
        in_specs=[pl.BlockSpec(memory_space=pltpu.SMEM)] + [whole] * (len(operands) - 1),
        out_specs=jax.tree.map(lambda _: whole, out_shape),
        scratch_shapes=scratch,
    )(*operands)


def array(shape, dtype=jnp.float32):
    return jax.ShapeDtypeStruct(shape, dtype)


def project_pieces(n, place_ref, zero, one, w_ref):
    width = zero[0].shape[1]
    rows = zero[0].shape[0] // n
    left = [
        jnp.concatenate([ref[...] for ref in zero], 1),
        jnp.concatenate(
            [
                jnp.concatenate([ref[k * rows : (k + 1) * rows] for k in range(n)], 1)
                for ref in one
            ],
            0,
        ),
    ]
    total = None
    for c in range(2):
        weights = []
        for k in range(n):
            x = lax.rem(place_ref[X] + n - k, n)
            for q in range(width // 128):
                start = pl.multiple_of(((c * (width // 128) + q) * n + x) * 128, 128)
                weights.append(w_ref[pl.ds(start, 128), :])
        weight = jnp.concatenate(weights, 0)
        product = jnp.dot(left[c], weight, preferred_element_type=jnp.float32)
        total = product if total is None else total + product
    return left, total


def conv_project_kernel(n, features, place_ref, *refs):
    pieces, w_ref, out_ref, scale_ref = refs[: 2 * n], refs[2 * n], refs[-2], refs[-1]

    def finish(zero, one):
        left, total = project_pieces(n, place_ref, zero, one, w_ref)
        rows = total.shape[0] // n
        for k in range(n):
            where = slice(k * rows, (k + 1) * rows)
            square = jnp.zeros((rows, 128), jnp.float32)
            for side in left:
                for f in range(side.shape[1] // 128):
                    wide = side[where, f * 128 : (f + 1) * 128].astype(jnp.float32)
                    square = square + wide * wide
            square = jnp.sum(square, axis=-1, keepdims=True)
            scale = lax.rsqrt(square * (1.0 / features) + 1e-06)
            scale_ref[where, :] = jnp.broadcast_to(scale, (rows, 128))
            block = total[where] * scale
            out_ref[lax.rem(place_ref[Y] + n - k, n)] = block.astype(jnp.bfloat16)

    pl.when(place_ref[C] == 0)(lambda: finish(pieces[:n], pieces[n:]))
    pl.when(place_ref[C] == 1)(lambda: finish(pieces[n:], pieces[:n]))


def gate_project_kernel(n, place_ref, *refs):
    pieces, w_ref, scale_ref, outs = refs[: 2 * n], refs[2 * n], refs[2 * n + 1], refs[2 * n + 2 :]

    def finish(zero, one):
        _, total = project_pieces(n, place_ref, zero, one, w_ref)
        rows = total.shape[0] // n
        for k in range(n):
            where = slice(k * rows + HALO, (k + 1) * rows)
            scale = scale_ref[where, :1]
            outs[k][...] = (total[where] * scale).astype(jnp.bfloat16)

    pl.when(place_ref[C] == 0)(lambda: finish(pieces[:n], pieces[n:]))
    pl.when(place_ref[C] == 1)(lambda: finish(pieces[n:], pieces[:n]))


def conv_kernel(place_ref, got_ref, w_ref, bias_ref, proj_ref, act_ref, kept_ref, given_ref, whole_ref):
    n, rows, width = got_ref.shape
    tokens = rows - HALO
    per = width // 128
    total = None
    for q in range(n):
        lanes = slice(q * width, (q + 1) * width)
        wide = got_ref[q].astype(jnp.float32)
        mixed = bias_ref[:, lanes]
        for tap in range(4):
            first = HALO - 3 + tap
            mixed = mixed + w_ref[tap : tap + 1, lanes] * wide[first : first + tokens]
        active = mixed * jax.nn.sigmoid(mixed)
        for h in range(per):
            for t in range(tokens // 8):
                row = (t * n * per + q * per + h) * 8
                act_ref[row : row + 8, :] = active[t * 8 : t * 8 + 8, h * 128 : h * 128 + 128]
        product = lax.dot_general(
            active.astype(jnp.bfloat16),
            proj_ref[:, lanes],
            (((1,), (1,)), ((), ())),
            preferred_element_type=jnp.float32,
        )
        total = product if total is None else total + product
    whole_ref[...] = total
    half = tokens // 2
    mine = place_ref[C]
    kept_ref[...] = whole_ref[pl.ds(pl.multiple_of(mine * half, half), half), :]
    given_ref[...] = whole_ref[pl.ds(pl.multiple_of((1 - mine) * half, half), half), :]


def joined_halves(place_ref, mine_ref, theirs_ref, all_ref):
    half = mine_ref.shape[0]
    mine = place_ref[C]
    all_ref[pl.ds(pl.multiple_of(mine * half, half), half), :] = mine_ref[...]
    all_ref[pl.ds(pl.multiple_of((1 - mine) * half, half), half), :] = theirs_ref[...]


def spread(all_ref, first, states, out_ref):
    tokens = all_ref.shape[0]
    tail = all_ref[:, first : first + states]
    for n in range(states):
        column = jnp.broadcast_to(tail[:, n : n + 1], (tokens, 128))
        out_ref[n * tokens : (n + 1) * tokens, :] = column


def scan_loop(tokens, states, begin, step_ref, act_ref, a_ref, b_ref, c_ref=None, emit=None):
    rates = [a_ref[n] for n in range(states)]

    def eight_tokens(tile, carry):
        state, steps = list(carry[0]), carry[1]
        for s in range(8):
            rows = pl.ds(tile * 64 + s, 8, stride=8)
            step, active = step_ref[rows, :], act_ref[rows, :]
            drive = step * active
            total = None
            for n in range(states):
                row = pl.ds(n * tokens + tile * 8 + s, 1)
                decay = jnp.exp2(step * rates[n])
                state[n] = decay * state[n] + drive * b_ref[row, :]
                if emit is not None:
                    part = state[n] * c_ref[row, :]
                    total = part if total is None else total + part
            if emit is not None:
                emit(rows, total, active)
            else:
                steps = steps + step
        return tuple(state), steps

    return lax.fori_loop(0, tokens // 8, eight_tokens, (begin, jnp.zeros((8, 128), jnp.float32)))


def store_packed(out_ref, steps, state):
    high = steps.astype(jnp.bfloat16)
    low = (steps - high.astype(jnp.float32)).astype(jnp.bfloat16)
    for copy in range(out_ref.shape[0]):
        out_ref[copy, 0] = high
        out_ref[copy, 1] = low
        for n, value in enumerate(state):
            out_ref[copy, 2 + n] = value.astype(jnp.bfloat16)


def steps_of(got_ref, k):
    return got_ref[k, 0].astype(jnp.float32) + got_ref[k, 1].astype(jnp.float32)


def prescan_kernel(
    place_ref, mine_ref, theirs_ref, dt_ref, bias_ref, act_ref, a_ref, step_ref, end_ref, all_ref, b_ref
):
    joined_halves(place_ref, mine_ref, theirs_ref, all_ref)
    tokens = all_ref.shape[0]
    rank, channels = dt_ref.shape
    states = a_ref.shape[0]
    spread(all_ref, rank, states, b_ref)
    raw = all_ref[:, :rank].astype(jnp.bfloat16)
    value = jnp.dot(raw, dt_ref[...], preferred_element_type=jnp.float32) + bias_ref[...]
    value = jnp.maximum(value, 0.0) + jnp.log1p(jnp.exp(-jnp.abs(value)))
    for t in range(tokens // 8):
        for j in range(channels // 128):
            row = (t * (channels // 128) + j) * 8
            step_ref[row : row + 8, :] = value[t * 8 : t * 8 + 8, j * 128 : j * 128 + 128]
    begin = tuple(jnp.zeros((8, 128), jnp.float32) for _ in range(states))
    final, steps = scan_loop(tokens, states, begin, step_ref, act_ref, a_ref, b_ref)
    store_packed(end_ref, steps, final)


def row_kernel(place_ref, got_ref, a_ref, inside_ref, whole_ref):
    states = a_ref.shape[0]
    zero = jnp.zeros(a_ref.shape[1:], jnp.float32)
    steps, state = zero, [zero] * states
    for k in range(got_ref.shape[0]):

        @pl.when(place_ref[Z] == k)
        def _(steps=steps, state=tuple(state)):
            for n in range(states):
                inside_ref[n] = state[n]
            inside_ref[states] = steps

        own = steps_of(got_ref, k)
        for n in range(states):
            end = got_ref[k, 2 + n].astype(jnp.float32)
            state[n] = jnp.exp2(a_ref[n] * own) * state[n] + end
        steps = steps + own
    store_packed(whole_ref, steps, state)


def rescan_kernel(n, place_ref, mine_ref, theirs_ref, step_ref, act_ref, a_ref, far_ref, near_ref, skip_ref, *refs):
    gates, out_ref = refs[:n], refs[n]
    all_ref, b_ref, c_ref, y_ref = refs[n + 1 :]
    joined_halves(place_ref, mine_ref, theirs_ref, all_ref)
    tokens, width = gates[0].shape
    states = a_ref.shape[0]
    first = all_ref.shape[1] - 2 * states
    spread(all_ref, first, states, b_ref)
    spread(all_ref, first + states, states, c_ref)
    skip = skip_ref[...]
    since = near_ref[states]
    begin = [jnp.zeros_like(since)] * states
    for k in range(far_ref.shape[0] - 1):
        before = k < place_ref[Y]
        own = steps_of(far_ref, k)
        for i in range(states):
            row = jnp.exp2(a_ref[i] * own) * begin[i] + far_ref[k, 2 + i].astype(jnp.float32)
            begin[i] = jnp.where(before, row, begin[i])
    begin = tuple(jnp.exp2(a_ref[i] * since) * begin[i] + near_ref[i] for i in range(states))

    def emit(rows, total, active):
        y_ref[rows, :] = total + skip * active

    scan_loop(tokens, states, begin, step_ref, act_ref, a_ref, b_ref, c_ref, emit)
    per = width // 128
    for k in range(n):
        q = lax.rem(place_ref[Y] + k, n)
        for h in range(per):
            gate = gates[k][:, h * 128 : h * 128 + 128].astype(jnp.float32)
            parts = []
            for t in range(tokens // 8):
                row = pl.multiple_of((t * n * per + q * per + h) * 8, 8)
                parts.append(y_ref[pl.ds(row, 8), :])
            value = jnp.concatenate(parts, 0) * (gate * jax.nn.sigmoid(gate))
            lanes = pl.ds(pl.multiple_of((q * per + h) * 128, 128), 128)
            out_ref[:, lanes] = value.astype(jnp.bfloat16)


def output_kernel(n, place_ref, *refs):
    pieces, w_ref, given_ref, kept_ref = refs[:n], refs[n], refs[n + 1], refs[n + 2]
    half = w_ref.shape[1] // 2
    rows = pieces[0].shape[0]
    left = jnp.concatenate([ref[...] for ref in pieces], 0)
    for out_ref, h in ((given_ref, 1 - place_ref[C]), (kept_ref, place_ref[C])):
        lanes = pl.ds(pl.multiple_of(h * half, half), half)
        product = jnp.dot(left, w_ref[:, lanes], preferred_element_type=jnp.float32)
        product = product.astype(jnp.bfloat16)
        for r in range(n):
            out_ref[r] = product[r * rows : (r + 1) * rows]


def pair_kernel(n, place_ref, kept_ref, got_ref, *outs):
    for k in range(n):
        r = lax.rem(place_ref[X] + 2 * n - place_ref[Y] - k, n)
        pair = kept_ref[r].astype(jnp.float32) + got_ref[r].astype(jnp.float32)
        outs[k][...] = pair.astype(jnp.bfloat16)


def spread_tokens(tokens):
    n = lax.axis_size("y")
    order = [(i, i + 1) for i in range(lax.axis_size(SEQ) - 1)]
    ahead = lax.ppermute(tokens[-HALO:], SEQ, order)
    block = jnp.concatenate([ahead, tokens], 0)
    for stage in range(2):
        got = [block]
        for k in range(1, n):
            route = []
            for y in range(n):
                for x in range(n):
                    for c in range(2):
                        to = ((y + k) % n, x) if c == stage else (y, (x + k) % n)
                        route.append(((y * n + x) * 2 + c, (to[0] * n + to[1]) * 2 + c))
            got.append(lax.ppermute(block, ("y", "x", "c"), route))
        block = jnp.concatenate(got, 0) if stage == 0 else got
    return block


def on_device(
    tokens,
    norm_gain,
    in_proj,
    conv_weight,
    conv_bias,
    x_proj,
    dt_proj,
    dt_bias,
    a_log,
    d_skip,
    out_proj,
):
    local_tokens = tokens.shape[0]
    channels = in_proj.shape[2]
    n = lax.axis_size("y")
    states = a_log.shape[1]
    features_out = x_proj.shape[1]
    tile_rows = local_tokens * channels // 128
    width = channels // n
    where = place()

    features = norm_gain.shape[0]
    count = in_proj.shape[0]
    gain = lax.dynamic_slice_in_dim(norm_gain, lax.axis_index(SEQ) * count, count, 0)
    gained = (in_proj.astype(jnp.float32) * gain[:, None, None]).astype(jnp.bfloat16)
    quarters = gained.reshape(-1, 2, n, width).transpose(2, 1, 0, 3)
    quarters = lax.all_to_all(quarters, "y", 0, 0, tiled=True)
    conv_w = lax.all_gather(quarters[:, 0].reshape(-1, width), "z", axis=0, tiled=True)
    gate_w = lax.all_gather(quarters[:, 1].reshape(-1, width), "z", axis=0, tiled=True)

    own = spread_tokens(tokens)
    pieces = own + [shifted(own[0], "c", 1)]
    pieces += [shifted(piece, "c", 1) for piece in own[1:]]
    rows = own[0].shape[0]
    conv_quad, scale = call(
        functools.partial(conv_project_kernel, n, features),
        (array((n, rows // n, width), jnp.bfloat16), array((rows, 128))),
        where,
        *pieces,
        conv_w,
    )
    conv_got = lax.all_to_all(conv_quad, "y", 0, 0, tiled=True)
    act_tiles, kept, given = call(
        conv_kernel,
        (
            array((tile_rows, 128)),
            array((local_tokens // 2, features_out)),
            array((local_tokens // 2, features_out)),
        ),
        where,
        conv_got,
        conv_weight,
        conv_bias.reshape(1, -1),
        x_proj.T,
        scratch=[pltpu.VMEM((local_tokens, features_out), jnp.float32)],
    )
    pair = kept + shifted(given, "c", 1)
    behind = from_behind(pair, "x")
    mine = sum(behind[1:], pair)
    theirs = shifted(mine, "c", 1)

    swap = [(y * n + x, x * n + y) for y in range(n) for x in range(n)]
    turned = lax.ppermute(out_proj, ("y", "x"), swap)
    out_w = lax.all_gather(turned, "z", axis=1, tiled=True)

    gate_quad = call(
        functools.partial(gate_project_kernel, n),
        tuple(array((local_tokens, width), jnp.bfloat16) for _ in range(n)),
        where,
        *pieces,
        gate_w,
        scale,
    )
    gate_got = given_back(gate_quad, "y")

    rates = (-LOG2E * jnp.exp(a_log)).T.reshape(states, channels // 128, 128)
    shard = (states + 2, *rates.shape[1:])
    all_features = pltpu.VMEM((local_tokens, features_out), jnp.float32)
    spread_rows = pltpu.VMEM((local_tokens * states, 128), jnp.float32)
    step_tiles, packed = call(
        prescan_kernel,
        (array((tile_rows, 128)), array((lax.axis_size("z"), *shard), jnp.bfloat16)),
        where,
        mine,
        theirs,
        dt_proj,
        dt_bias.reshape(1, -1),
        act_tiles,
        rates,
        scratch=[all_features, spread_rows],
    )
    ends = lax.all_to_all(packed, "z", 0, 0, tiled=True)
    near, whole = call(
        row_kernel,
        (array((states + 1, *rates.shape[1:])), array((n, *shard), jnp.bfloat16)),
        where,
        ends,
        rates,
    )
    far = lax.all_to_all(whole, "y", 0, 0, tiled=True)
    gated = call(
        functools.partial(rescan_kernel, n),
        array((local_tokens, channels), jnp.bfloat16),
        where,
        mine,
        theirs,
        step_tiles,
        act_tiles,
        rates,
        far,
        near,
        d_skip.reshape(channels // 128, 128),
        *gate_got,
        scratch=[all_features, spread_rows, spread_rows, pltpu.VMEM((tile_rows, 128), jnp.float32)],
    )

    held = [
        lax.ppermute(
            gated,
            ("y", "x"),
            [(y * n + x, x * n + (y + r) % n) for y in range(n) for x in range(n)],
        )
        for r in range(n)
    ]
    half = array((n, local_tokens, out_w.shape[1] // 2), jnp.bfloat16)
    given, kept = call(functools.partial(output_kernel, n), (half, half), where, *held, out_w)
    sent = call(
        functools.partial(pair_kernel, n),
        tuple(array(half.shape[1:], jnp.bfloat16) for _ in range(n)),
        where,
        kept,
        shifted(given, "c", 1),
    )
    arrived = [sent[0]] + [shifted(sent[k], "y", k) for k in range(1, n)]
    mixed = sum((piece.astype(jnp.float32) for piece in arrived[1:]), arrived[0].astype(jnp.float32))
    return mixed.astype(jnp.bfloat16)


def solution(mesh):
    torus = Mesh(mesh.devices.reshape(4, 8, 4, 2), ("y", "z", "x", "c"))
    return jax.shard_map(
        on_device,
        mesh=torus,
        in_specs=(
            P(SEQ, CH),
            P(),
            P(SEQ, None, CH),
            P(None, CH),
            P(CH),
            P(CH, None),
            P(None, CH),
            P(CH),
            P(CH, None),
            P(CH),
            P(CH, SEQ),
        ),
        out_specs=P(SEQ, CH),
        check_vma=False,
    )
```

```python
import functools

import jax
import jax.numpy as jnp
from jax import lax
from jax.experimental import pallas as pl
from jax.experimental.pallas import tpu as pltpu
from jax.sharding import Mesh
from jax.sharding import PartitionSpec as P


SEQ = ("y", "z")
CH = ("x", "c")
HALO = 16
AXES = ("y", "z", "x", "c")
Y, Z, X, C = range(4)
LOG2E = 1.4426950408889634


def shifted(block, axis, distance):
    n = lax.axis_size(axis)
    return lax.ppermute(block, axis, [(i, (i + distance) % n) for i in range(n)])


def from_behind(block, axis):
    return [block] + [shifted(block, axis, k) for k in range(1, lax.axis_size(axis))]


def given_back(pieces, axis):
    return [pieces[0]] + [shifted(pieces[k], axis, -k) for k in range(1, len(pieces))]


def place():
    return jnp.stack([lax.axis_index(axis) for axis in AXES]).astype(jnp.int32)


def call(kernel, out_shape, *operands, scratch=()):
    whole = pl.BlockSpec(memory_space=pltpu.VMEM)
    return pl.pallas_call(
        kernel,
        out_shape=out_shape,
        in_specs=[pl.BlockSpec(memory_space=pltpu.SMEM)] + [whole] * (len(operands) - 1),
        out_specs=jax.tree.map(lambda _: whole, out_shape),
        scratch_shapes=scratch,
    )(*operands)


def array(shape, dtype=jnp.float32):
    return jax.ShapeDtypeStruct(shape, dtype)


def project_pieces(n, place_ref, zero, one, w_ref, by_distance):
    width = zero[0].shape[1]
    rows = zero[0].shape[0] // n
    left = [
        jnp.concatenate([ref[...] for ref in zero], 1),
        jnp.concatenate(
            [
                jnp.concatenate([ref[k * rows : (k + 1) * rows] for k in range(n)], 1)
                for ref in one
            ],
            0,
        ),
    ]
    total = None
    for c in range(2):
        weights = []
        for k in range(n):
            x = lax.rem(place_ref[X] + n - k, n)
            at = lax.rem(place_ref[Y] + n - x, n) if by_distance else x
            for q in range(width // 128):
                start = pl.multiple_of(((c * (width // 128) + q) * n + at) * 128, 128)
                weights.append(w_ref[pl.ds(start, 128), :])
        weight = jnp.concatenate(weights, 0)
        product = jnp.dot(left[c], weight, preferred_element_type=jnp.float32)
        total = product if total is None else total + product
    return left, total


def conv_project_kernel(n, features, place_ref, *refs):
    pieces, w_ref, out_ref, scale_ref = refs[: 2 * n], refs[2 * n], refs[-2], refs[-1]

    def finish(zero, one):
        left, total = project_pieces(n, place_ref, zero, one, w_ref, True)
        rows = total.shape[0] // n
        for k in range(n):
            where = slice(k * rows, (k + 1) * rows)
            square = jnp.zeros((rows, 128), jnp.float32)
            for side in left:
                for f in range(side.shape[1] // 128):
                    wide = side[where, f * 128 : (f + 1) * 128].astype(jnp.float32)
                    square = square + wide * wide
            square = jnp.sum(square, axis=-1, keepdims=True)
            scale = lax.rsqrt(square * (1.0 / features) + 1e-06)
            scale_ref[where, :] = jnp.broadcast_to(scale, (rows, 128))
            block = total[where] * scale
            out_ref[lax.rem(place_ref[Y] + n - k, n)] = block.astype(jnp.bfloat16)

    pl.when(place_ref[C] == 0)(lambda: finish(pieces[:n], pieces[n:]))
    pl.when(place_ref[C] == 1)(lambda: finish(pieces[n:], pieces[:n]))


def gate_project_kernel(n, place_ref, *refs):
    pieces, w_ref, scale_ref, outs = refs[: 2 * n], refs[2 * n], refs[2 * n + 1], refs[2 * n + 2 :]

    def finish(zero, one):
        _, total = project_pieces(n, place_ref, zero, one, w_ref, False)
        rows = total.shape[0] // n
        for k in range(n):
            where = slice(k * rows + HALO, (k + 1) * rows)
            scale = scale_ref[where, :1]
            outs[k][...] = (total[where] * scale).astype(jnp.bfloat16)

    pl.when(place_ref[C] == 0)(lambda: finish(pieces[:n], pieces[n:]))
    pl.when(place_ref[C] == 1)(lambda: finish(pieces[n:], pieces[:n]))


def conv_kernel(place_ref, got_ref, w_ref, bias_ref, proj_ref, act_ref, kept_ref, given_ref, whole_ref):
    n, rows, width = got_ref.shape
    tokens = rows - HALO
    per = width // 128
    total = None
    for q in range(n):
        lanes = slice(q * width, (q + 1) * width)
        wide = got_ref[q].astype(jnp.float32)
        mixed = bias_ref[:, lanes]
        for tap in range(4):
            first = HALO - 3 + tap
            mixed = mixed + w_ref[tap : tap + 1, lanes] * wide[first : first + tokens]
        active = mixed * jax.nn.sigmoid(mixed)
        for h in range(per):
            for t in range(tokens // 8):
                row = (t * n * per + q * per + h) * 8
                act_ref[row : row + 8, :] = active[t * 8 : t * 8 + 8, h * 128 : h * 128 + 128]
        product = lax.dot_general(
            active.astype(jnp.bfloat16),
            proj_ref[:, lanes],
            (((1,), (1,)), ((), ())),
            preferred_element_type=jnp.float32,
        )
        total = product if total is None else total + product
    whole_ref[...] = total
    half = tokens // 2
    mine = place_ref[C]
    kept_ref[...] = whole_ref[pl.ds(pl.multiple_of(mine * half, half), half), :]
    given_ref[...] = whole_ref[pl.ds(pl.multiple_of((1 - mine) * half, half), half), :]


def joined_halves(place_ref, mine_ref, theirs_ref, all_ref):
    half = mine_ref.shape[0]
    mine = place_ref[C]
    all_ref[pl.ds(pl.multiple_of(mine * half, half), half), :] = mine_ref[...]
    all_ref[pl.ds(pl.multiple_of((1 - mine) * half, half), half), :] = theirs_ref[...]


def spread(all_ref, first, states, out_ref):
    tokens = all_ref.shape[0]
    tail = all_ref[:, first : first + states]
    for n in range(states):
        column = jnp.broadcast_to(tail[:, n : n + 1], (tokens, 128))
        out_ref[n * tokens : (n + 1) * tokens, :] = column


def scan_loop(tokens, states, begin, step_ref, act_ref, a_ref, b_ref, c_ref=None, emit=None):
    rates = [a_ref[n] for n in range(states)]

    def eight_tokens(tile, carry):
        state, steps = list(carry[0]), carry[1]
        for s in range(8):
            rows = pl.ds(tile * 64 + s, 8, stride=8)
            step, active = step_ref[rows, :], act_ref[rows, :]
            drive = step * active
            total = None
            for n in range(states):
                row = pl.ds(n * tokens + tile * 8 + s, 1)
                decay = jnp.exp2(step * rates[n])
                state[n] = decay * state[n] + drive * b_ref[row, :]
                if emit is not None:
                    part = state[n] * c_ref[row, :]
                    total = part if total is None else total + part
            if emit is not None:
                emit(rows, total, active)
            else:
                steps = steps + step
        return tuple(state), steps

    return lax.fori_loop(0, tokens // 8, eight_tokens, (begin, jnp.zeros((8, 128), jnp.float32)))


def store_packed(out_ref, steps, state):
    high = steps.astype(jnp.bfloat16)
    low = (steps - high.astype(jnp.float32)).astype(jnp.bfloat16)
    for copy in range(out_ref.shape[0]):
        out_ref[copy, 0] = high
        out_ref[copy, 1] = low
        for n, value in enumerate(state):
            out_ref[copy, 2 + n] = value.astype(jnp.bfloat16)


def steps_of(got_ref, k):
    return got_ref[k, 0].astype(jnp.float32) + got_ref[k, 1].astype(jnp.float32)


def prescan_kernel(
    place_ref, mine_ref, theirs_ref, dt_ref, bias_ref, act_ref, a_ref, step_ref, end_ref, all_ref, b_ref
):
    joined_halves(place_ref, mine_ref, theirs_ref, all_ref)
    tokens = all_ref.shape[0]
    rank, channels = dt_ref.shape
    states = a_ref.shape[0]
    spread(all_ref, rank, states, b_ref)
    raw = all_ref[:, :rank].astype(jnp.bfloat16)
    value = jnp.dot(raw, dt_ref[...], preferred_element_type=jnp.float32) + bias_ref[...]
    value = jnp.maximum(value, 0.0) + jnp.log1p(jnp.exp(-jnp.abs(value)))
    for t in range(tokens // 8):
        for j in range(channels // 128):
            row = (t * (channels // 128) + j) * 8
            step_ref[row : row + 8, :] = value[t * 8 : t * 8 + 8, j * 128 : j * 128 + 128]
    begin = tuple(jnp.zeros((8, 128), jnp.float32) for _ in range(states))
    final, steps = scan_loop(tokens, states, begin, step_ref, act_ref, a_ref, b_ref)
    store_packed(end_ref, steps, final)


def row_kernel(place_ref, got_ref, a_ref, inside_ref, whole_ref):
    states = a_ref.shape[0]
    zero = jnp.zeros(a_ref.shape[1:], jnp.float32)
    steps, state = zero, [zero] * states
    for k in range(got_ref.shape[0]):

        @pl.when(place_ref[Z] == k)
        def _(steps=steps, state=tuple(state)):
            for n in range(states):
                inside_ref[n] = state[n]
            inside_ref[states] = steps

        own = steps_of(got_ref, k)
        for n in range(states):
            end = got_ref[k, 2 + n].astype(jnp.float32)
            state[n] = jnp.exp2(a_ref[n] * own) * state[n] + end
        steps = steps + own
    store_packed(whole_ref, steps, state)


def rescan_kernel(n, place_ref, mine_ref, theirs_ref, step_ref, act_ref, a_ref, far_ref, near_ref, skip_ref, *refs):
    gates, out_ref = refs[:n], refs[n]
    all_ref, b_ref, c_ref, y_ref = refs[n + 1 :]
    joined_halves(place_ref, mine_ref, theirs_ref, all_ref)
    tokens, width = gates[0].shape
    states = a_ref.shape[0]
    first = all_ref.shape[1] - 2 * states
    spread(all_ref, first, states, b_ref)
    spread(all_ref, first + states, states, c_ref)
    skip = skip_ref[...]
    since = near_ref[states]
    begin = [jnp.zeros_like(since)] * states
    for k in range(far_ref.shape[0] - 1):
        before = k < place_ref[Y]
        own = steps_of(far_ref, k)
        for i in range(states):
            row = jnp.exp2(a_ref[i] * own) * begin[i] + far_ref[k, 2 + i].astype(jnp.float32)
            begin[i] = jnp.where(before, row, begin[i])
    begin = tuple(jnp.exp2(a_ref[i] * since) * begin[i] + near_ref[i] for i in range(states))

    def emit(rows, total, active):
        y_ref[rows, :] = total + skip * active

    scan_loop(tokens, states, begin, step_ref, act_ref, a_ref, b_ref, c_ref, emit)
    per = width // 128
    for k in range(n):
        q = lax.rem(place_ref[Y] + k, n)
        for h in range(per):
            gate = gates[k][:, h * 128 : h * 128 + 128].astype(jnp.float32)
            parts = []
            for t in range(tokens // 8):
                row = pl.multiple_of((t * n * per + q * per + h) * 8, 8)
                parts.append(y_ref[pl.ds(row, 8), :])
            value = jnp.concatenate(parts, 0) * (gate * jax.nn.sigmoid(gate))
            lanes = pl.ds(pl.multiple_of((q * per + h) * 128, 128), 128)
            out_ref[:, lanes] = value.astype(jnp.bfloat16)


def output_kernel(n, place_ref, *refs):
    pieces, w_ref, given_ref, kept_ref = refs[:n], refs[n], refs[n + 1], refs[n + 2]
    half = w_ref.shape[1] // 2
    rows = pieces[0].shape[0]
    left = jnp.concatenate([ref[...] for ref in pieces], 0)
    for out_ref, h in ((given_ref, 1 - place_ref[C]), (kept_ref, place_ref[C])):
        lanes = pl.ds(pl.multiple_of(h * half, half), half)
        product = jnp.dot(left, w_ref[:, lanes], preferred_element_type=jnp.float32)
        product = product.astype(jnp.bfloat16)
        for r in range(n):
            out_ref[r] = product[r * rows : (r + 1) * rows]


def pair_kernel(n, place_ref, kept_ref, got_ref, *outs):
    for k in range(n):
        r = lax.rem(place_ref[X] + 2 * n - place_ref[Y] - k, n)
        pair = kept_ref[r].astype(jnp.float32) + got_ref[r].astype(jnp.float32)
        outs[k][...] = pair.astype(jnp.bfloat16)


def spread_tokens(tokens):
    n = lax.axis_size("y")
    order = [(i, i + 1) for i in range(lax.axis_size(SEQ) - 1)]
    ahead = lax.ppermute(tokens[-HALO:], SEQ, order)
    block = jnp.concatenate([ahead, tokens], 0)
    for stage in range(2):
        got = [block]
        for k in range(1, n):
            route = []
            for y in range(n):
                for x in range(n):
                    for c in range(2):
                        to = ((y + k) % n, x) if c == stage else (y, (x + k) % n)
                        route.append(((y * n + x) * 2 + c, (to[0] * n + to[1]) * 2 + c))
            got.append(lax.ppermute(block, ("y", "x", "c"), route))
        block = jnp.concatenate(got, 0) if stage == 0 else got
    return block


def on_device(
    tokens,
    norm_gain,
    in_proj,
    conv_weight,
    conv_bias,
    x_proj,
    dt_proj,
    dt_bias,
    a_log,
    d_skip,
    out_proj,
):
    local_tokens = tokens.shape[0]
    channels = in_proj.shape[2]
    n = lax.axis_size("y")
    states = a_log.shape[1]
    features_out = x_proj.shape[1]
    tile_rows = local_tokens * channels // 128
    width = channels // n
    where = place()

    features = norm_gain.shape[0]
    count = in_proj.shape[0]
    first = lax.axis_index(SEQ) * count
    gain = lax.dynamic_slice_in_dim(norm_gain, first, count, 0)
    gained = (in_proj.astype(jnp.float32) * gain[:, None, None]).astype(jnp.bfloat16)
    conv_part = gained[:, 0]
    mine = lax.axis_index("y")
    parts = [
        lax.dynamic_slice_in_dim(conv_part, (mine + k) % n * width, width, 1) for k in range(n)
    ]
    parts[1:] = [shifted(parts[k], "y", k) for k in range(1, n)]
    conv_w = lax.all_gather(jnp.concatenate(parts, 0), "z", axis=0, tiled=True)
    gate_part = gained[:, 1].reshape(count, n, width).transpose(1, 0, 2)
    gate_part = lax.all_to_all(gate_part, "y", 0, 0, tiled=True)
    gate_w = lax.all_gather(gate_part.reshape(-1, width), "z", axis=0, tiled=True)

    own = spread_tokens(tokens)
    pieces = own + [shifted(own[0], "c", 1)]
    pieces += [shifted(piece, "c", 1) for piece in own[1:]]
    rows = own[0].shape[0]
    conv_quad, scale = call(
        functools.partial(conv_project_kernel, n, features),
        (array((n, rows // n, width), jnp.bfloat16), array((rows, 128))),
        where,
        *pieces,
        conv_w,
    )
    conv_got = lax.all_to_all(conv_quad, "y", 0, 0, tiled=True)
    act_tiles, kept, given = call(
        conv_kernel,
        (
            array((tile_rows, 128)),
            array((local_tokens // 2, features_out)),
            array((local_tokens // 2, features_out)),
        ),
        where,
        conv_got,
        conv_weight,
        conv_bias.reshape(1, -1),
        x_proj.T,
        scratch=[pltpu.VMEM((local_tokens, features_out), jnp.float32)],
    )
    pair = kept + shifted(given, "c", 1)
    behind = from_behind(pair.astype(jnp.bfloat16), "x")
    mine = sum((piece.astype(jnp.float32) for piece in behind[1:]), pair)
    theirs = shifted(mine, "c", 1)

    swap = [(y * n + x, x * n + y) for y in range(n) for x in range(n)]
    turned = lax.ppermute(out_proj, ("y", "x"), swap)
    out_w = lax.all_gather(turned, "z", axis=1, tiled=True)

    gate_quad = call(
        functools.partial(gate_project_kernel, n),
        tuple(array((local_tokens, width), jnp.bfloat16) for _ in range(n)),
        where,
        *pieces,
        gate_w,
        scale,
    )
    gate_got = given_back(gate_quad, "y")

    rates = (-LOG2E * jnp.exp(a_log)).T.reshape(states, channels // 128, 128)
    shard = (states + 2, *rates.shape[1:])
    all_features = pltpu.VMEM((local_tokens, features_out), jnp.float32)
    spread_rows = pltpu.VMEM((local_tokens * states, 128), jnp.float32)
    step_tiles, packed = call(
        prescan_kernel,
        (array((tile_rows, 128)), array((lax.axis_size("z"), *shard), jnp.bfloat16)),
        where,
        mine,
        theirs,
        dt_proj,
        dt_bias.reshape(1, -1),
        act_tiles,
        rates,
        scratch=[all_features, spread_rows],
    )
    ends = lax.all_to_all(packed, "z", 0, 0, tiled=True)
    near, whole = call(
        row_kernel,
        (array((states + 1, *rates.shape[1:])), array((n, *shard), jnp.bfloat16)),
        where,
        ends,
        rates,
    )
    far = lax.all_to_all(whole, "y", 0, 0, tiled=True)
    gated = call(
        functools.partial(rescan_kernel, n),
        array((local_tokens, channels), jnp.bfloat16),
        where,
        mine,
        theirs,
        step_tiles,
        act_tiles,
        rates,
        far,
        near,
        d_skip.reshape(channels // 128, 128),
        *gate_got,
        scratch=[all_features, spread_rows, spread_rows, pltpu.VMEM((tile_rows, 128), jnp.float32)],
    )

    held = [
        lax.ppermute(
            gated,
            ("y", "x"),
            [(y * n + x, x * n + (y + r) % n) for y in range(n) for x in range(n)],
        )
        for r in range(n)
    ]
    half = array((n, local_tokens, out_w.shape[1] // 2), jnp.bfloat16)
    given, kept = call(functools.partial(output_kernel, n), (half, half), where, *held, out_w)
    sent = call(
        functools.partial(pair_kernel, n),
        tuple(array(half.shape[1:], jnp.bfloat16) for _ in range(n)),
        where,
        kept,
        shifted(given, "c", 1),
    )
    arrived = [sent[0]] + [shifted(sent[k], "y", k) for k in range(1, n)]
    mixed = sum((piece.astype(jnp.float32) for piece in arrived[1:]), arrived[0].astype(jnp.float32))
    return mixed.astype(jnp.bfloat16)


def solution(mesh):
    torus = Mesh(mesh.devices.reshape(4, 8, 4, 2), ("y", "z", "x", "c"))
    return jax.shard_map(
        on_device,
        mesh=torus,
        in_specs=(
            P(SEQ, CH),
            P(),
            P(SEQ, None, CH),
            P(None, CH),
            P(CH),
            P(CH, None),
            P(None, CH),
            P(CH),
            P(CH, None),
            P(CH),
            P(CH, SEQ),
        ),
        out_specs=P(SEQ, CH),
        check_vma=False,
    )
```
